32 devices in a mesh: wl: 8 (over y, x, core), tile: 4 (over z).
Axes of the slice: x: 2, y: 2, z: 4, core: 2. Of those that a mesh axis runs over, the one named last changes fastest.
Arguments:
- forward: float32 [32, 2, 1024, 1024], P(('wl', 'tile')), may hold values from -6 to 6
- adjoint: float32 [32, 2, 1024, 1024], P(('wl', 'tile')), may hold values from -6 to 6
- mode: float32 [2, 1024], replicated, may hold values from -6 to 6
- target: float32 [32], P(('wl', 'tile')), may hold values from 0 to 2
- wl_index: int32 [32], P(('wl', 'tile')), may hold values from 0 to 31, each once
- tile_of: int32 [32], replicated, may hold values from 0 to 31, each once
- density: float32 [1024, 1024], P(('wl', 'tile')), may hold values from 0 to 1
Outputs:
- gradient: float32 [1024, 1024], P(('wl', 'tile'))
The draws below stay inside these ranges and needn't reach their ends.
All inputs are finite; a program needn't handle non-finite values.
Results may differ from the reference program's by a relative error of at most 0.00002.
Values sent between devices are 32-bit elements; how exact they have to be, the bound alone decides.
A program may use at most 64 MiB of HBM per device.

```python
import jax
import jax.numpy as jnp
from jax import lax

ROWS = 1024
COLS = 1024
NWL = 32
N_WL = 8
N_TILE = 4
DEVICES = 32


def block_scale(key, shape, cuts, least, high):
    def one(dim, shards_of):
        steps = jax.random.uniform(jax.random.fold_in(jax.random.fold_in(key, 6), dim), (shards_of,), jnp.float32, least / len(cuts), high / len(cuts))
        return jnp.repeat(jnp.exp(steps), shape[dim] // shards_of).reshape((-1,) + (1,) * (len(shape) - dim - 1))

    loudness = one(*cuts[0])
    for cut in cuts[1:]:
        loudness = loudness * one(*cut)
    return loudness


def bell_draw(own_key, dims, spread, most, shards=(), kind=jnp.bfloat16):
    loudness = block_scale(own_key, dims, shards, -0.22, 0.18) if shards else 1.0
    result = jax.random.normal(own_key, dims, jnp.float32) * spread * loudness
    return jnp.minimum(jnp.maximum(result, -most), most).astype(kind)


def setup_inputs(seed: int = 0) -> dict:
    key_list = jax.random.split(jax.random.key(seed), 8)
    return {
        "forward": bell_draw(key_list[0], (NWL, 2, ROWS, COLS), 1.0, 6.0, ((0, 32),), jnp.float32),
        "adjoint": bell_draw(key_list[1], (NWL, 2, ROWS, COLS), 1.0, 6.0, ((0, 32),), jnp.float32),
        "mode": bell_draw(key_list[2], (2, COLS), 1.0, 6.0, (), jnp.float32),
        "target": jnp.clip(2.0 * jax.random.uniform(key_list[3], (NWL,), jnp.float32) ** block_scale(key_list[3], (NWL,), ((0, 32),), -0.2, 0.2), 0.0, 2.0),
        "wl_index": jax.random.permutation(key_list[4], NWL).astype(jnp.int32),
        "tile_of": jax.random.permutation(key_list[5], DEVICES).astype(jnp.int32),
        "density": jnp.clip(1.0 * jax.random.uniform(key_list[6], (ROWS, COLS), jnp.float32) ** block_scale(key_list[6], (ROWS, COLS), ((0, 32),), -0.2, 0.2), 0.0, 1.0),
    }


def reference(forward, adjoint, mode, target, wl_index, tile_of, density):
    devices = N_WL * N_TILE
    mon = ROWS // 2
    line = forward[:, :, mon, :]
    over_re = lax.optimization_barrier(jnp.sum(line[:, 0] * mode[0] - line[:, 1] * mode[1], axis=1))
    over_im = lax.optimization_barrier(jnp.sum(line[:, 0] * mode[1] + line[:, 1] * mode[0], axis=1))
    fom = (over_re * over_re + over_im * over_im) / COLS
    scale = jnp.sum(fom) / NWL + 1.0
    weight = target - fom / scale
    freq = 1.0 + wl_index.astype(jnp.float32) / NWL

    def accumulate(total, items):
        fwd, adj, wgt, frq = items
        field = frq * frq * (fwd[0] * adj[0] - fwd[1] * adj[1])
        return (total + wgt * field, None)
    start = jnp.zeros((ROWS, COLS), jnp.float32)
    total, _ = lax.scan(accumulate, start, (forward, adjoint, weight, freq))
    tile_rows = ROWS // devices
    arranged = total.reshape(devices, tile_rows, COLS)[tile_of].reshape(ROWS, COLS)
    slope = 4.0 * (1.0 - jnp.tanh(4.0 * (density - 0.5)) ** 2)
    shaped = arranged * slope
    return shaped / jnp.sqrt(jnp.mean(shaped * shaped) + 1e-06)
```

```python
import functools

import jax
import jax.numpy as jnp
from jax import lax
from jax.experimental import pallas as pl
from jax.experimental.pallas import tpu as pltpu
from jax.sharding import PartitionSpec as P

MESH = pl.DeviceIdType.MESH
SUB = 8
LANES = 128
PIECES = 8


def plane(wide):
    cores = 2 if wide % 2 == 0 else 1
    chips = wide // cores
    first = max(f for f in range(1, chips + 1) if chips % f == 0 and f * f <= chips)
    return first, chips // first, cores


def kernel(
    sizes, tile_of, target, wl_index, mode, density, fwd, adj, shaped_out, squares_out,
    line, f_src, f_recv, q_src, q_recv, slope, own, away, r0, r1, r2, r3,
    in_sem, f_ssem, f_rsem, q_ssem, q_rsem, s0, e0, s1, e1, s2, e2, s3, e3, *bufs,
):
    g1, g2, cores, deep, groups, parts, rows, cols = sizes
    wide = g1 * g2 * cores
    devices = wide * deep
    tile_rows = rows // devices
    per_core = g1 * g2 * deep
    width = cols // parts
    f_bufs, a_bufs = bufs[:groups], bufs[groups:]
    w_me, z_me = lax.axis_index("wl"), lax.axis_index("tile")
    me = w_me * deep + z_me
    c_me = w_me % cores
    b_me = (w_me // cores) % g2
    a_me = w_me // (cores * g2)

    def at(a, b, c, z):
        return ((a * g2 + b) * cores + c, z)

    def everyone(o):
        f = (me + o) % devices
        return (f // deep, f % deep)

    mon = rows // 2
    mt, mk, ms = mon // tile_rows, (mon % tile_rows) // SUB, mon % SUB
    line_copy = pltpu.make_async_copy(fwd.at[:, mt, mk], line, in_sem.at[2 * groups])
    line_copy.start()
    loads = []
    for k in range(groups):
        pair = (
            pltpu.make_async_copy(fwd.at[:, :, k], f_bufs[k], in_sem.at[2 * k]),
            pltpu.make_async_copy(adj.at[:, :, k], a_bufs[k], in_sem.at[2 * k + 1]),
        )
        for copy in pair:
            copy.start()
        loads.append(pair)

    barrier = pltpu.get_barrier_semaphore()

    @pl.loop(1, devices)
    def _(o):
        pl.semaphore_signal(barrier, inc=1, device_id=everyone(o), device_id_type=MESH)

    line_copy.wait()
    re, im = line[0, ms : ms + 1, :], line[1, ms : ms + 1, :]
    m_re, m_im = mode[0:1, :], mode[1:2, :]
    over_re = jnp.sum(re * m_re - im * m_im, axis=1, keepdims=True)
    over_im = jnp.sum(re * m_im + im * m_re, axis=1, keepdims=True)
    fom = jnp.broadcast_to((over_re * over_re + over_im * over_im) / cols, (1, LANES))
    f_src[...] = fom

    pl.semaphore_wait(barrier, devices - 1)

    def share(src, recv, ssem, rsem):
        def copy(o):
            return pltpu.make_async_remote_copy(
                src_ref=src, dst_ref=recv.at[o - 1],
                send_sem=ssem.at[o - 1], recv_sem=rsem.at[o - 1],
                device_id=everyone(o), device_id_type=MESH,
            )

        @pl.loop(1, devices)
        def _(o):
            copy(o).start()

        return copy

    f_copy = share(f_src, f_recv, f_ssem, f_rsem)
    slope[...] = 4.0 * (1.0 - jnp.tanh(4.0 * (density[...] - 0.5)) ** 2)

    def finish(copy):
        @pl.loop(1, devices)
        def _(o):
            copy(o).wait()

    finish(f_copy)
    total_fom = fom + jnp.sum(f_recv[...], axis=0)
    scale = total_fom / devices + 1.0
    weight = target[0] - fom / scale
    freq = 1.0 + wl_index[0].astype(jnp.float32) / devices
    factor = jnp.max(weight) * freq * freq

    def order(piece):
        return (g1, g2) if piece % 2 == 0 else (g2, g1)

    def build(k):
        for copy in loads[k]:
            copy.wait()
        for half in range(cores):

            @pl.loop(0, per_core)
            def _(i):
                oz = i % deep
                hi, lo = (i // deep) // g2, (i // deep) % g2
                c = (c_me + half) % cores
                z = (z_me + oz) % deep
                d = ((((a_me + hi) % g1) * g2 + (b_me + lo) % g2) * cores + c) * deep + z
                t = tile_of[d]
                slot = ((lo * g1) + hi) * deep + oz
                for p in range(parts):
                    cs = slice(p * width, (p + 1) * width)
                    value = factor * (
                        f_bufs[k][0, t, :, cs] * a_bufs[k][0, t, :, cs]
                        - f_bufs[k][1, t, :, cs] * a_bufs[k][1, t, :, cs]
                    )
                    piece = k * parts + p
                    where = i if piece % 2 == 0 else slot
                    if half == 0:
                        own[piece, where] = value
                    else:
                        away[piece, where] = value

    def swap(piece):
        return pltpu.make_async_remote_copy(
            src_ref=away.at[piece], dst_ref=r0.at[piece],
            send_sem=s0.at[piece], recv_sem=e0.at[piece],
            device_id=at(a_me, b_me, (c_me + 1) % cores, z_me), device_id_type=MESH,
        )

    def scatter(piece, step):
        n1, n2 = order(piece)
        n = (n1, n2, deep)[step]
        span = (n2 * deep, deep, 1)[step]
        recv, ssem, rsem = ((r1, s1, e1), (r2, s2, e2), (r3, s3, e3))[step]
        axis = step if step == 2 else (step + piece) % 2
        copies = []
        for o in range(1, n):
            where = (
                at((a_me + o) % g1, b_me, c_me, z_me) if axis == 0
                else at(a_me, (b_me + o) % g2, c_me, z_me) if axis == 1
                else at(a_me, b_me, c_me, (z_me + o) % deep)
            )
            copies.append(pltpu.make_async_remote_copy(
                src_ref=own.at[piece, pl.ds(o * span, span)],
                dst_ref=recv.at[piece, pl.ds((o - 1) * span, span)],
                send_sem=ssem.at[piece, o - 1], recv_sem=rsem.at[piece, o - 1],
                device_id=where, device_id_type=MESH,
            ))
        return copies, recv, span, n

    def start(piece, step):
        for copy in scatter(piece, step)[0]:
            copy.start()

    def add(piece, step):
        copies, recv, span, n = scatter(piece, step)
        for copy in copies:
            copy.wait_recv()

        @pl.loop(0, span)
        def _(i):
            value = own[piece, i]
            for o in range(n - 1):
                value = value + recv[piece, o * span + i]
            own[piece, i] = value

    pieces = groups * parts

    def first(piece):
        if cores > 1:
            swap(piece).wait_recv()

            @pl.loop(0, per_core)
            def _(i):
                own[piece, i] = own[piece, i] + r0[piece, i]

        start(piece, 0)

    built = 0
    for turn in range(pieces // 2 + 3):
        def open_pair(pair):
            nonlocal built
            while built * parts < 2 * pair + 2:
                build(built)
                if cores > 1:
                    for p in range(parts):
                        swap(built * parts + p).start()
                built += 1
            for piece in (2 * pair, 2 * pair + 1):
                first(piece)

        if turn == 0:
            open_pair(0)
            if pieces // 2 > 1:
                open_pair(1)
        if turn < pieces // 2:
            for piece in (2 * turn, 2 * turn + 1):
                add(piece, 0)
                start(piece, 1)
            if turn + 2 < pieces // 2:
                open_pair(turn + 2)
        if 1 <= turn <= pieces // 2:
            for piece in (2 * turn - 2, 2 * turn - 1):
                add(piece, 1)
                start(piece, 2)

    squares = jnp.zeros((1, 1), jnp.float32)
    for piece in range(pieces):
        copies, recv, span, n = scatter(piece, 2)
        for copy in copies:
            copy.wait_recv()
        value = own[piece, 0]
        for o in range(n - 1):
            value = value + recv[piece, o]
        k, p = piece // parts, piece % parts
        rs, cs = slice(k * SUB, (k + 1) * SUB), slice(p * width, (p + 1) * width)
        shaped = value * slope[rs, cs]
        shaped_out[rs, cs] = shaped
        squares = squares + jnp.sum(shaped * shaped, keepdims=True)
    mine = jnp.broadcast_to(squares, (1, LANES))
    q_src[...] = mine
    q_copy = share(q_src, q_recv, q_ssem, q_rsem)

    for piece in range(pieces):
        if cores > 1:
            swap(piece).wait_send()
        for step in range(3):
            for copy in scatter(piece, step)[0]:
                copy.wait_send()
    finish(q_copy)
    squares_out[...] = mine + jnp.sum(q_recv[...], axis=0)


def per_device(forward, adjoint, mode, target, wl_index, tile_of, density):
    wide, deep = lax.axis_size("wl"), lax.axis_size("tile")
    devices = wide * deep
    rows, cols = forward.shape[2:]
    g1, g2, cores = plane(wide)
    tile_rows = rows // devices
    groups = tile_rows // SUB
    parts = max(1, min(PIECES // groups, cols // LANES))
    pieces = groups * parts
    width = cols // parts
    per_core = g1 * g2 * deep
    fwd = forward.reshape(2, devices, groups, SUB, cols)
    adj = adjoint.reshape(2, devices, groups, SUB, cols)
    f32 = jnp.float32
    dma = pltpu.SemaphoreType.DMA
    most = max(g1, g2, 2) - 1
    block = lambda n: pltpu.VMEM((pieces, max(n, 1), SUB, width), f32)
    sizes = (g1, g2, cores, deep, groups, parts, rows, cols)
    peers = max(devices - 1, 1)
    vmem = pl.BlockSpec(memory_space=pltpu.VMEM)
    smem = pl.BlockSpec(memory_space=pltpu.SMEM)
    hbm = pl.BlockSpec(memory_space=pl.ANY)
    third = max(deep - 1, 1)
    shaped, squares = pl.pallas_call(
        functools.partial(kernel, sizes),
        out_shape=(
            jax.ShapeDtypeStruct((tile_rows, cols), f32),
            jax.ShapeDtypeStruct((1, LANES), f32),
        ),
        in_specs=[smem, smem, smem, vmem, vmem, hbm, hbm],
        out_specs=(vmem, vmem),
        scratch_shapes=[
            pltpu.VMEM((2, SUB, cols), f32),
            pltpu.VMEM((1, LANES), f32),
            pltpu.VMEM((peers, 1, LANES), f32),
            pltpu.VMEM((1, LANES), f32),
            pltpu.VMEM((peers, 1, LANES), f32),
            pltpu.VMEM((tile_rows, cols), f32),
            block(per_core),
            block(per_core),
            block(per_core),
            block(per_core),
            block(per_core // min(g1, g2)),
            block(third),
            dma((2 * groups + 1,)),
            dma((peers,)), dma((peers,)), dma((peers,)), dma((peers,)),
            dma((pieces,)), dma((pieces,)),
            dma((pieces, most)), dma((pieces, most)),
            dma((pieces, most)), dma((pieces, most)),
            dma((pieces, third)), dma((pieces, third)),
        ]
        + [pltpu.VMEM((2, devices, SUB, cols), f32)] * (2 * groups),
        compiler_params=pltpu.CompilerParams(
            collective_id=0, has_side_effects=True, vmem_limit_bytes=60 * 2**20
        ),
        name="assemble",
    )(tile_of, target, wl_index, mode, density, fwd, adj)
    return shaped / jnp.sqrt(squares[0, 0] / (rows * cols) + 1e-06)


def solution(mesh):
    in_specs = (
        P(("wl", "tile"), None, None, None),
        P(("wl", "tile"), None, None, None),
        P(),
        P(("wl", "tile")),
        P(("wl", "tile")),
        P(),
        P(("wl", "tile"), None),
    )
    out_specs = P(("wl", "tile"), None)
    return jax.shard_map(
        per_device, mesh=mesh, in_specs=in_specs, out_specs=out_specs, check_vma=False
    )
```

```python
import functools

import jax
import jax.numpy as jnp
from jax import lax
from jax.experimental import pallas as pl
from jax.experimental.pallas import tpu as pltpu
from jax.sharding import PartitionSpec as P

MESH = pl.DeviceIdType.MESH
SUB = 8
LANES = 128
PIECES = 16
AHEAD = 3


def plane(wide):
    cores = 2 if wide % 2 == 0 else 1
    chips = wide // cores
    first = max(f for f in range(1, chips + 1) if chips % f == 0 and f * f <= chips)
    return first, chips // first, cores


def kernel(
    sizes, pair_in, tiles_in, mode_in, density_in, fwd, adj, shaped_hbm, norm_out,
    own_pair, tile_of, mode, density, shaped_out,
    line, f_src, f_recv, q_src, q_recv, slope, own, away, r0, r1, r2, r3,
    in_sem, side_sem, f_ssem, f_rsem, q_ssem, q_rsem, s0, e0, s1, e1, s2, e2, s3, e3, *bufs,
):
    g1, g2, cores, deep, groups, parts, rows, cols = sizes
    wide = g1 * g2 * cores
    devices = wide * deep
    tile_rows = rows // devices
    per_core = g1 * g2 * deep
    width = cols // parts
    f_bufs, a_bufs = bufs[:groups], bufs[groups:]
    w_me, z_me = lax.axis_index("wl"), lax.axis_index("tile")
    me = w_me * deep + z_me
    c_me = w_me % cores
    b_me = (w_me // cores) % g2
    a_me = w_me // (cores * g2)

    def at(a, b, c, z):
        return ((a * g2 + b) * cores + c, z)

    def everyone(o):
        f = (me + o) % devices
        return (f // deep, f % deep)

    barrier = pltpu.get_barrier_semaphore()

    @pl.loop(1, devices)
    def _(o):
        pl.semaphore_signal(barrier, inc=1, device_id=everyone(o), device_id_type=MESH)

    mon = rows // 2
    mt, mk, ms = mon // tile_rows, (mon % tile_rows) // SUB, mon % SUB
    line_copy = pltpu.make_async_copy(fwd.at[:, mt, mk], line, in_sem.at[2 * groups])
    mode_copy = pltpu.make_async_copy(mode_in, mode, side_sem.at[0])
    tile_copy = pltpu.make_async_copy(tiles_in, tile_of, side_sem.at[1])
    density_copy = pltpu.make_async_copy(density_in, density, side_sem.at[2])
    pair_copy = pltpu.make_async_copy(pair_in, own_pair, side_sem.at[4])
    for copy in (line_copy, mode_copy, tile_copy, density_copy, pair_copy):
        copy.start()
    loads = []
    for k in range(groups):
        pair = (
            pltpu.make_async_copy(fwd.at[:, :, k], f_bufs[k], in_sem.at[2 * k]),
            pltpu.make_async_copy(adj.at[:, :, k], a_bufs[k], in_sem.at[2 * k + 1]),
        )
        if k == 0:
            for copy in pair:
                copy.start()
        loads.append(pair)

    line_copy.wait()
    mode_copy.wait()
    re, im = line[0, ms : ms + 1, :], line[1, ms : ms + 1, :]
    m_re, m_im = mode[0:1, :], mode[1:2, :]
    over_re = jnp.sum(re * m_re - im * m_im, axis=1, keepdims=True)
    over_im = jnp.sum(re * m_im + im * m_re, axis=1, keepdims=True)
    fom = jnp.broadcast_to((over_re * over_re + over_im * over_im) / cols, (1, LANES))
    f_src[...] = fom

    pl.semaphore_wait(barrier, devices - 1)

    def share(src, recv, ssem, rsem):
        def copy(o):
            return pltpu.make_async_remote_copy(
                src_ref=src, dst_ref=recv.at[o - 1],
                send_sem=ssem.at[o - 1], recv_sem=rsem.at[o - 1],
                device_id=everyone(o), device_id_type=MESH,
            )

        @pl.loop(1, devices)
        def _(o):
            copy(o).start()

        return copy

    f_copy = share(f_src, f_recv, f_ssem, f_rsem)
    for pair in loads[1:]:
        for copy in pair:
            copy.start()
    density_copy.wait()
    slope[...] = 4.0 * (1.0 - jnp.tanh(4.0 * (density[...] - 0.5)) ** 2)

    def finish(copy):
        @pl.loop(1, devices)
        def _(o):
            copy(o).wait()

    finish(f_copy)
    total_fom = fom + jnp.sum(f_recv[...], axis=0)
    scale = total_fom / devices + 1.0
    pair_copy.wait()
    weight = own_pair[0] - fom / scale
    freq = 1.0 + own_pair[1] / devices
    factor = jnp.concatenate([weight * freq * freq] * (width // LANES), axis=1)
    factor = jnp.broadcast_to(factor, (SUB, width))
    tile_copy.wait()

    def order(piece):
        return (g1, g2) if piece % 2 == 0 else (g2, g1)

    def build(k):
        for copy in loads[k]:
            copy.wait()
        for half in range(cores):

            @pl.loop(0, g1 * g2)
            def _(i):
                hi, lo = i // g2, i % g2
                c = (c_me + half) % cores
                base = ((((a_me + hi) % g1) * g2 + (b_me + lo) % g2) * cores + c) * deep
                slots = (i * deep, (lo * g1 + hi) * deep)
                for oz in range(deep):
                    t = tile_of[base + (z_me + oz) % deep]
                    for p in range(parts):
                        cs = slice(p * width, (p + 1) * width)
                        piece = k * parts + p
                        (away if half else own)[piece, slots[piece % 2] + oz] = factor * (
                            f_bufs[k][0, t, :, cs] * a_bufs[k][0, t, :, cs]
                            - f_bufs[k][1, t, :, cs] * a_bufs[k][1, t, :, cs]
                        )

    def swap(piece):
        return pltpu.make_async_remote_copy(
            src_ref=away.at[piece], dst_ref=r0.at[piece],
            send_sem=s0.at[piece], recv_sem=e0.at[piece],
            device_id=at(a_me, b_me, (c_me + 1) % cores, z_me), device_id_type=MESH,
        )

    def scatter(piece, step):
        n1, n2 = order(piece)
        n = (n1, n2, deep)[step]
        span = (n2 * deep, deep, 1)[step]
        recv, ssem, rsem = ((r1, s1, e1), (r2, s2, e2), (r3, s3, e3))[step]
        axis = step if step == 2 else (step + piece) % 2
        copies = []
        for o in range(1, n):
            where = (
                at((a_me + o) % g1, b_me, c_me, z_me) if axis == 0
                else at(a_me, (b_me + o) % g2, c_me, z_me) if axis == 1
                else at(a_me, b_me, c_me, (z_me + o) % deep)
            )
            copies.append(pltpu.make_async_remote_copy(
                src_ref=own.at[piece, pl.ds(o * span, span)],
                dst_ref=recv.at[piece, pl.ds((o - 1) * span, span)],
                send_sem=ssem.at[piece, o - 1], recv_sem=rsem.at[piece, o - 1],
                device_id=where, device_id_type=MESH,
            ))
        return copies, recv, span, n

    def start(piece, step):
        for copy in scatter(piece, step)[0]:
            copy.start()

    def add(piece, step):
        copies, recv, span, n = scatter(piece, step)
        for copy in copies:
            copy.wait_recv()

        value = own[piece, :span]
        for o in range(n - 1):
            value = value + recv[piece, o * span : (o + 1) * span]
        own[piece, :span] = value

    pieces = groups * parts

    def first(piece):
        if cores > 1:
            swap(piece).wait_recv()
            own[piece] = own[piece] + r0[piece]

        start(piece, 0)

    built = 0

    def make(upto):
        nonlocal built
        while built < min(upto, groups):
            build(built)
            if cores > 1:
                for p in range(parts):
                    swap(built * parts + p).start()
            built += 1

    def open_pair(pair):
        make((2 * pair + 1) // parts + 2)
        for piece in (2 * pair, 2 * pair + 1):
            first(piece)

    for turn in range(pieces // 2 + 1):
        if turn == 0:
            for pair in range(min(AHEAD, pieces // 2)):
                open_pair(pair)
        if turn < pieces // 2:
            for piece in (2 * turn, 2 * turn + 1):
                add(piece, 0)
                start(piece, 1)
            if turn + AHEAD < pieces // 2:
                open_pair(turn + AHEAD)
        if 1 <= turn <= pieces // 2:
            for piece in (2 * turn - 2, 2 * turn - 1):
                add(piece, 1)
                start(piece, 2)

    squares = jnp.zeros((1, 1), jnp.float32)
    for piece in range(pieces):
        copies, recv, span, n = scatter(piece, 2)
        for copy in copies:
            copy.wait_recv()
        value = own[piece, 0]
        for o in range(n - 1):
            value = value + recv[piece, o]
        k, p = piece // parts, piece % parts
        rs, cs = slice(k * SUB, (k + 1) * SUB), slice(p * width, (p + 1) * width)
        shaped = value * slope[rs, cs]
        shaped_out[rs, cs] = shaped
        squares = squares + jnp.sum(shaped * shaped, keepdims=True)
    out_copy = pltpu.make_async_copy(shaped_out, shaped_hbm, side_sem.at[3])
    out_copy.start()
    mine = jnp.broadcast_to(squares, (1, LANES))
    q_src[...] = mine
    q_copy = share(q_src, q_recv, q_ssem, q_rsem)

    for piece in range(pieces):
        if cores > 1:
            swap(piece).wait_send()
        for step in range(3):
            for copy in scatter(piece, step)[0]:
                copy.wait_send()
    out_copy.wait()
    finish(q_copy)
    squares = mine + jnp.sum(q_recv[...], axis=0)
    norm_out[...] = jnp.sqrt(squares / (rows * cols) + 1e-06)


def per_device(forward, adjoint, mode, target, wl_index, tile_of, density):
    wide, deep = lax.axis_size("wl"), lax.axis_size("tile")
    devices = wide * deep
    rows, cols = forward.shape[2:]
    g1, g2, cores = plane(wide)
    tile_rows = rows // devices
    groups = tile_rows // SUB
    parts = max(1, min(PIECES // groups, cols // LANES))
    pieces = groups * parts
    width = cols // parts
    per_core = g1 * g2 * deep
    fwd = forward.reshape(2, devices, groups, SUB, cols)
    adj = adjoint.reshape(2, devices, groups, SUB, cols)
    f32 = jnp.float32
    dma = pltpu.SemaphoreType.DMA
    most = max(g1, g2, 2) - 1
    block = lambda n: pltpu.VMEM((pieces, max(n, 1), SUB, width), f32)
    sizes = (g1, g2, cores, deep, groups, parts, rows, cols)
    peers = max(devices - 1, 1)
    vmem = pl.BlockSpec(memory_space=pltpu.VMEM)
    hbm = pl.BlockSpec(memory_space=pl.ANY)
    third = max(deep - 1, 1)
    shaped, norm = pl.pallas_call(
        functools.partial(kernel, sizes),
        out_shape=(
            jax.ShapeDtypeStruct((tile_rows, cols), f32),
            jax.ShapeDtypeStruct((1, LANES), f32),
        ),
        in_specs=[hbm, hbm, hbm, hbm, hbm, hbm],
        out_specs=(hbm, vmem),
        scratch_shapes=[
            pltpu.SMEM((2,), f32),
            pltpu.SMEM((devices,), jnp.int32),
            pltpu.VMEM(mode.shape, f32),
            pltpu.VMEM((tile_rows, cols), f32),
            pltpu.VMEM((tile_rows, cols), f32),
            pltpu.VMEM((2, SUB, cols), f32),
            pltpu.VMEM((1, LANES), f32),
            pltpu.VMEM((peers, 1, LANES), f32),
            pltpu.VMEM((1, LANES), f32),
            pltpu.VMEM((peers, 1, LANES), f32),
            pltpu.VMEM((tile_rows, cols), f32),
            block(per_core),
            block(per_core),
            block(per_core),
            block(per_core),
            block(per_core // min(g1, g2)),
            block(third),
            dma((2 * groups + 1,)),
            dma((5,)),
            dma((peers,)), dma((peers,)), dma((peers,)), dma((peers,)),
            dma((pieces,)), dma((pieces,)),
            dma((pieces, most)), dma((pieces, most)),
            dma((pieces, most)), dma((pieces, most)),
            dma((pieces, third)), dma((pieces, third)),
        ]
        + [pltpu.VMEM((2, devices, SUB, cols), f32)] * (2 * groups),
        compiler_params=pltpu.CompilerParams(
            collective_id=0, has_side_effects=True, vmem_limit_bytes=60 * 2**20
        ),
        name="assemble",
    )(jnp.concatenate([target, wl_index.astype(f32)]), tile_of, mode, density, fwd, adj)
    return shaped / norm[0, 0]


def solution(mesh):
    in_specs = (
        P(("wl", "tile"), None, None, None),
        P(("wl", "tile"), None, None, None),
        P(),
        P(("wl", "tile")),
        P(("wl", "tile")),
        P(),
        P(("wl", "tile"), None),
    )
    out_specs = P(("wl", "tile"), None)
    return jax.shard_map(
        per_device, mesh=mesh, in_specs=in_specs, out_specs=out_specs, check_vma=False
    )
```
